32 devices in a mesh: cut: 8 (over z, y), sub: 4 (over x, core).
Axes of the slice: x: 2, y: 2, z: 4, core: 2. Of those that a mesh axis runs over, the one named last changes fastest.
Arguments:
- residual: bfloat16 [8, 4, 1024, 128], P('cut', 'sub'), may hold values from -6 to 6
- inner_inverse: bfloat16 [8, 4, 4, 343, 343], P('cut', 'sub'), may hold values from -0.3125 to 0.3125
- inner_index: int32 [8, 4, 4, 343], P('cut', 'sub'), may hold values from 0 to 1023
- slab_dofs: int32 [8, 4, 5, 512], P('cut', 'sub'), may hold values from 0 to 1023
- face_inverse: bfloat16 [8, 4, 5, 3, 343, 343], P('cut', 'sub'), may hold values from -0.3125 to 0.3125
- face_index: int32 [8, 4, 5, 3, 343], P('cut', 'sub'), may hold values from 0 to 1023
- face_count: int32 [8, 4, 5], P('cut', 'sub'), may hold values from 1 to 3
Outputs:
- correction: float32 [8, 4, 1024, 128], P('cut', 'sub')
The draws below stay inside these ranges and needn't reach their ends.
All inputs are finite; a program needn't handle non-finite values.
Results may differ from the reference program's by a relative error of at most 0.0003.
Values may be sent and summed in bfloat16 or wider, within the bound.
A program may use at most 64 MiB of HBM per device.

```python
import jax
import jax.numpy as jnp
from jax import lax

STAR = 343
NDOF = 1024
NRHS = 128
NINT = 4
SLAB = 512
ISTAR = 3
CUTLV = 3
LEVELS = 5
PC = 8
PS = 4
N_CUT = 8
N_SUB = 4


def set_ends(entries, key, least, top_value):
    index_at = [jax.random.randint(jax.random.fold_in(key, axis), (), 0, length) for axis, length in enumerate(entries.shape)]
    longest = entries.shape.index(max(entries.shape))
    beside = index_at[:longest] + [(index_at[longest] + 1) % entries.shape[longest]] + index_at[longest + 1:]
    return entries.at[tuple(index_at)].set(least).at[tuple(beside)].set(top_value)


def shard_levels(stream_key, shape, shards, least, high):
    level = 1.0
    for axis_at, blocks in shards:
        heights = jax.random.uniform(jax.random.fold_in(jax.random.fold_in(stream_key, 6), axis_at), (blocks,), jnp.float32, least / len(shards), high / len(shards))
        level = level * jnp.repeat(jnp.exp(heights), shape[axis_at] // blocks).reshape((-1,) + (1,) * (len(shape) - 1 - axis_at))
    return level


def gaussian(key, extent, scale, bound, pieces=(), kind=jnp.bfloat16):
    drawn = scale * jax.random.normal(key, extent, jnp.float32)
    if pieces:
        drawn = drawn * shard_levels(key, extent, pieces, -0.22, 0.18)
    return jnp.clip(drawn, -bound, bound).astype(kind)


def setup_inputs(seed: int = 0) -> dict:
    keys = jax.random.split(jax.random.key(seed), 8)
    return {
        "residual": gaussian(keys[0], (PC, PS, NDOF, NRHS), 1.0, 6.0, ((0, 8), (1, 4))),
        "inner_inverse": gaussian(keys[1], (PC, PS, NINT, STAR, STAR), STAR ** -0.5, 0.3125, ((0, 8), (1, 4))),
        "inner_index": set_ends(jax.random.randint(keys[2], (PC, PS, NINT, STAR), 0, NDOF), jax.random.fold_in(keys[2], 1), 0, NDOF - 1).astype(jnp.int32),
        "slab_dofs": set_ends(jax.random.randint(keys[3], (PC, PS, LEVELS, SLAB), 0, NDOF), jax.random.fold_in(keys[3], 1), 0, NDOF - 1).astype(jnp.int32),
        "face_inverse": gaussian(keys[4], (PC, PS, LEVELS, ISTAR, STAR, STAR), STAR ** -0.5, 0.3125, ((0, 8), (1, 4))),
        "face_index": set_ends(jax.random.randint(keys[5], (PC, PS, LEVELS, ISTAR, STAR), 0, 2 * SLAB), jax.random.fold_in(keys[5], 1), 0, (2 * SLAB) - 1).astype(jnp.int32),
        "face_count": set_ends(jax.random.randint(keys[6], (PC, PS, LEVELS), 1, ISTAR + 1), jax.random.fold_in(keys[6], 1), 1, ISTAR).astype(jnp.int32),
    }


def star_apply(inverses, indices, live, source, row_count):
    gathered = jnp.take(source, indices, axis=0)
    solved = jnp.einsum("nij,njr->nir", inverses.astype(jnp.float32), gathered.astype(jnp.float32))
    solved = solved * live[:, None, None]
    width = source.shape[1]
    blank = jnp.zeros((row_count, width), jnp.float32)
    return blank.at[indices.reshape(-1)].add(solved.reshape(-1, width))


def reference(residual, inner_inverse, inner_index, slab_dofs, face_inverse, face_index, face_count):
    total_devices = PC * PS
    flat_residual = residual.reshape(total_devices, NDOF, NRHS)
    flat_inner_inv = inner_inverse.reshape(total_devices, NINT, STAR, STAR)
    flat_inner_idx = inner_index.reshape(total_devices, NINT, STAR)
    flat_dofs = slab_dofs.reshape(total_devices, LEVELS, SLAB)
    flat_face_inv = face_inverse.reshape(total_devices, LEVELS, ISTAR, STAR, STAR)
    flat_face_idx = face_index.reshape(total_devices, LEVELS, ISTAR, STAR)
    flat_count = face_count.reshape(total_devices, LEVELS)
    inner_live = jnp.ones((NINT,), jnp.float32)

    def inner_one(bundle):
        return star_apply(bundle[0], bundle[1], inner_live, bundle[2], NDOF)

    correction = lax.map(inner_one, (flat_inner_inv, flat_inner_idx, flat_residual))
    devices = jnp.arange(total_devices, dtype=jnp.int32)
    cut_index = devices // PS
    sub_index = devices % PS
    cut_bits = N_CUT.bit_length() - 1
    sub_bits = N_SUB.bit_length() - 1
    star_slots = jnp.arange(ISTAR, dtype=jnp.int32)
    for level in range(LEVELS):
        if level < CUTLV:
            shift_bit = cut_bits - 1 - level
            partner = (cut_index ^ (1 << shift_bit)) * PS + sub_index
            is_upper = (cut_index >> shift_bit) & 1
        else:
            shift_bit = sub_bits - 1 - (level - CUTLV)
            partner = cut_index * PS + (sub_index ^ (1 << shift_bit))
            is_upper = (sub_index >> shift_bit) & 1
        dofs_now = flat_dofs[:, level]
        own_slab = jax.vmap(lambda source, picked: jnp.take(source, picked, axis=0))(flat_residual, dofs_now)
        far_slab = own_slab[partner]
        upper_flag = (is_upper == 1)[:, None, None]
        joined = jnp.where(upper_flag, jnp.concatenate([far_slab, own_slab], axis=1), jnp.concatenate([own_slab, far_slab], axis=1))
        live = (star_slots[None, :] < flat_count[:, level][:, None]).astype(jnp.float32)

        def face_one(bundle):
            return star_apply(bundle[0], bundle[1], bundle[2], bundle[3], 2 * SLAB)

        terms = lax.map(face_one, (flat_face_inv[:, level], flat_face_idx[:, level], live, joined))
        paired = terms + terms[partner]
        slab_terms = jnp.where(upper_flag, paired[:, SLAB:], paired[:, :SLAB])
        correction = jax.vmap(lambda whole, picked, portion: whole.at[picked].add(portion))(correction, dofs_now, slab_terms)
    return correction.reshape(PC, PS, NDOF, NRHS)
```

```python
import jax
import jax.numpy as jnp
from jax import lax
from jax.experimental import pallas as pl
from jax.experimental.pallas import tpu as pltpu
from jax.sharding import PartitionSpec as P

CUTLV = 3
LANES = 128
CHUNK = 128
MESH = pl.DeviceIdType.MESH


def round_up(value, step):
    return (value + step - 1) // step * step


def split_pair(values):
    high = values.astype(jnp.bfloat16)
    low = (values - high.astype(jnp.float32)).astype(jnp.bfloat16)
    return high, low


def make_kernel(ndof, nrhs, nint, star, levels, slots, slab, order):
    pad = round_up(star, LANES)
    joint = 2 * slab

    def kernel(
        res, inner_inv, inner_idx, dofs, face_inv, face_idx, counts, out,
        inv_in, inv_face, rows, row_t, dof_t,
        pick, s_in, st_in, s_face, st_face, p_t,
        gathered, pair, joined, terms, back, acc,
        inv_sem, send_sem, recv_sem, give_sem, back_sem,
    ):
        copies = [pltpu.make_async_copy(inner_inv.at[0, 0], inv_in, inv_sem.at[levels])]
        for k in range(levels):
            copies.append(
                pltpu.make_async_copy(face_inv.at[0, 0, k], inv_face.at[k], inv_sem.at[k])
            )
        for copy in copies:
            copy.start()

        places = []
        for k in range(levels):
            axis = "cut" if k < CUTLV else "sub"
            bits = lax.axis_size(axis).bit_length() - 1
            apart = bits - 1 - (k if k < CUTLV else k - CUTLV)
            me = lax.axis_index(axis)
            upper = lax.rem(lax.div(me, 1 << apart), 2)
            far = me + (1 - 2 * upper) * (1 << apart)
            own_at = pl.multiple_of(upper * slab, slab)
            far_at = pl.multiple_of((1 - upper) * slab, slab)
            places.append(({axis: far}, own_at, far_at))

        barrier = pltpu.get_barrier_semaphore()
        for target, _, _ in places:
            pl.semaphore_signal(barrier, inc=1, device_id=target, device_id_type=MESH)

        rows[...] = jnp.full(rows.shape, -1, jnp.int32)
        rows[0:nint, 0:star] = inner_idx[0, 0]
        for k in range(levels):
            for j in range(slots):
                at = nint + k * slots + j
                live = j < counts[0, 0, k]
                rows[at : at + 1, 0:star] = jnp.where(live, face_idx[0, 0, k, j : j + 1], -1)
        row_t[...] = rows[...].T
        dof_rows = jnp.concatenate(
            [dofs[0, 0], jnp.full((round_up(levels, 8) - levels, slab), -1, jnp.int32)], axis=0
        )
        dof_t[...] = dof_rows.T

        def across(column, width):
            spots = lax.broadcasted_iota(jnp.int32, (column.shape[0], width), 1)
            return jnp.where(column == spots, 1.0, 0.0).astype(jnp.bfloat16)

        def down(row, first, height):
            spots = lax.broadcasted_iota(jnp.int32, (height, row.shape[1]), 0) + first
            return jnp.where(row == spots, 1.0, 0.0).astype(jnp.bfloat16)

        send, give = [], []
        for k, (target, own_at, far_at) in enumerate(places):
            send.append(
                pltpu.make_async_remote_copy(
                    src_ref=joined.at[k, pl.ds(own_at, slab)],
                    dst_ref=joined.at[k, pl.ds(own_at, slab)],
                    send_sem=send_sem.at[k],
                    recv_sem=recv_sem.at[k],
                    device_id=target,
                    device_id_type=MESH,
                )
            )
            give.append(
                pltpu.make_async_remote_copy(
                    src_ref=terms.at[k, pl.ds(far_at, slab)],
                    dst_ref=back.at[k],
                    send_sem=give_sem.at[k],
                    recv_sem=back_sem.at[k],
                    device_id=target,
                    device_id_type=MESH,
                )
            )

        for k, (_, own_at, _) in enumerate(places):
            for first in range(0, slab, CHUNK):
                pick[first : first + CHUNK] = across(dof_t[first : first + CHUNK, k : k + 1], ndof)
            mine = jnp.dot(pick[...], res[0, 0], preferred_element_type=jnp.float32)
            joined[k, pl.ds(own_at, slab)] = mine.astype(jnp.bfloat16)
            if k == 1:
                pl.semaphore_wait(barrier, levels)
            if k >= 1:
                send[k - 1].start()

        def build_down(target, row_of, count, height):
            def step(i, carry):
                first = pl.multiple_of(i * CHUNK, CHUNK)
                for j in range(count):
                    row = rows[row_of + j : row_of + j + 1, :]
                    target[pl.ds(first, CHUNK), j * pad : (j + 1) * pad] = down(row, first, CHUNK)
                return carry

            lax.fori_loop(0, height // CHUNK, step, 0)

        def build_across(target, row_of, count, width):
            for j in range(count):
                for first in range(0, pad, CHUNK):
                    column = row_t[first : first + CHUNK, row_of + j : row_of + j + 1]
                    target[j * pad + first : j * pad + first + CHUNK, :] = across(column, width)

        build_across(s_in, 0, nint, ndof)
        send[levels - 1].start()
        build_down(st_in, 0, nint, ndof)

        def solve(selector, source, inverses, count):
            gathered[0 : count * pad] = jnp.dot(
                selector, source, preferred_element_type=jnp.float32
            ).astype(jnp.bfloat16)
            for j in range(count):
                solved = jnp.dot(
                    inverses[j],
                    gathered[j * pad : j * pad + star],
                    preferred_element_type=jnp.float32,
                )
                high, low = split_pair(solved)
                pair[j * pad : j * pad + star, 0:nrhs] = high
                pair[j * pad : j * pad + star, nrhs : 2 * nrhs] = low

        pair[...] = jnp.zeros(pair.shape, jnp.bfloat16)
        copies[0].wait()
        solve(s_in[...], res[0, 0], inv_in, nint)
        acc[...] = jnp.dot(
            st_in[...], pair[0 : nint * pad], preferred_element_type=jnp.float32
        )

        for k in order:
            build_across(s_face.at[k], nint + k * slots, slots, joint)
            build_down(st_face.at[k], nint + k * slots, slots, joint)

        for k in range(levels):
            def step(i, carry):
                first = pl.multiple_of(i * CHUNK, CHUNK)
                p_t[k, pl.ds(first, CHUNK), :] = down(dofs[0, 0, k : k + 1, :], first, CHUNK)
                return carry

            lax.fori_loop(0, ndof // CHUNK, step, 0)

        for k in order:
            _, own_at, far_at = places[k]
            send[k].wait_recv()
            copies[1 + k].wait()
            solve(s_face[k], joined[k], inv_face.at[k], slots)
            for at in (far_at, own_at):
                both = jnp.dot(
                    st_face[k, pl.ds(at, slab), :],
                    pair[0 : slots * pad],
                    preferred_element_type=jnp.float32,
                )
                terms[k, pl.ds(at, slab), :] = both[:, :nrhs] + both[:, nrhs:]
            give[k].start()

        for k in order:
            _, own_at, _ = places[k]
            give[k].wait_recv()
            high, low = split_pair(terms[k, pl.ds(own_at, slab), :] + back[k])
            pair[0:slab, 0:nrhs] = high
            pair[0:slab, nrhs : 2 * nrhs] = low
            acc[...] += jnp.dot(p_t[k], pair[0:slab], preferred_element_type=jnp.float32)
        out[0, 0] = acc[:, :nrhs] + acc[:, nrhs:]
        for k in range(levels):
            send[k].wait_send()
            give[k].wait_send()

    return kernel


def on_device(
    residual, inner_inverse, inner_index, slab_dofs, face_inverse, face_index, face_count
):
    ndof, nrhs = residual.shape[2:]
    nint, star = inner_index.shape[2:]
    levels, slots = face_index.shape[2:4]
    slab = slab_dofs.shape[3]
    pad = round_up(star, LANES)
    joint = 2 * slab
    index_rows = round_up(nint + levels * slots, 8)
    order = (4, 3, 2, 0, 1)
    kinds = jnp.bfloat16
    vmem = pl.BlockSpec(memory_space=pltpu.VMEM)
    anywhere = pl.BlockSpec(memory_space=pl.ANY)
    scalar = pl.BlockSpec(memory_space=pltpu.SMEM)
    return pl.pallas_call(
        make_kernel(ndof, nrhs, nint, star, levels, slots, slab, order),
        out_shape=jax.ShapeDtypeStruct(residual.shape, jnp.float32),
        in_specs=[vmem, anywhere, vmem, vmem, anywhere, vmem, scalar],
        out_specs=vmem,
        scratch_shapes=[
            pltpu.VMEM((nint, star, star), kinds),
            pltpu.VMEM((levels, slots, star, star), kinds),
            pltpu.VMEM((index_rows, pad), jnp.int32),
            pltpu.VMEM((pad, index_rows), jnp.int32),
            pltpu.VMEM((slab, round_up(levels, 8)), jnp.int32),
            pltpu.VMEM((slab, ndof), kinds),
            pltpu.VMEM((nint * pad, ndof), kinds),
            pltpu.VMEM((ndof, nint * pad), kinds),
            pltpu.VMEM((levels, slots * pad, joint), kinds),
            pltpu.VMEM((levels, joint, slots * pad), kinds),
            pltpu.VMEM((levels, ndof, slab), kinds),
            pltpu.VMEM((max(nint, slots) * pad, nrhs), kinds),
            pltpu.VMEM((max(nint, slots) * pad, 2 * nrhs), kinds),
            pltpu.VMEM((levels, joint, nrhs), kinds),
            pltpu.VMEM((levels, joint, nrhs), jnp.float32),
            pltpu.VMEM((levels, slab, nrhs), jnp.float32),
            pltpu.VMEM((ndof, 2 * nrhs), jnp.float32),
            pltpu.SemaphoreType.DMA((levels + 1,)),
            pltpu.SemaphoreType.DMA((levels,)),
            pltpu.SemaphoreType.DMA((levels,)),
            pltpu.SemaphoreType.DMA((levels,)),
            pltpu.SemaphoreType.DMA((levels,)),
        ],
        compiler_params=pltpu.CompilerParams(
            collective_id=0, has_side_effects=True, vmem_limit_bytes=64000000
        ),
    )(residual, inner_inverse, inner_index, slab_dofs, face_inverse, face_index, face_count)


def solution(mesh):
    return jax.shard_map(
        on_device,
        mesh=mesh,
        in_specs=(
            P("cut", "sub", None, None),
            P("cut", "sub", None, None, None),
            P("cut", "sub", None, None),
            P("cut", "sub", None, None),
            P("cut", "sub", None, None, None, None),
            P("cut", "sub", None, None, None),
            P("cut", "sub", None),
        ),
        out_specs=P("cut", "sub", None, None),
        check_vma=False,
    )
```

```python
import jax
import jax.numpy as jnp
from jax import lax
from jax.experimental import pallas as pl
from jax.experimental.pallas import tpu as pltpu
from jax.sharding import PartitionSpec as P

CUTLV = 3
LANES = 128
CHUNK = 128
INDEX = jnp.int16
MESH = pl.DeviceIdType.MESH


def round_up(value, step):
    return (value + step - 1) // step * step


def split_pair(values):
    high = values.astype(jnp.bfloat16)
    low = (values - high.astype(jnp.float32)).astype(jnp.bfloat16)
    return high, low


def make_kernel(ndof, nrhs, nint, star, levels, slots, slab, early, order, finish):
    pad = round_up(star, LANES)
    joint = 2 * slab

    def kernel(
        res, inner_inv, inner_idx, dofs, face_inv, face_idx, counts, out,
        inv_in, inv_face, rows, res_t, st_in, st_face, p_t,
        gathered, pair, joined, terms, back, acc,
        inv_sem, send_sem, recv_sem, give_sem, back_sem,
    ):
        copies = [pltpu.make_async_copy(inner_inv.at[0, 0], inv_in, inv_sem.at[levels])]
        for k in range(levels):
            copies.append(
                pltpu.make_async_copy(face_inv.at[0, 0, k], inv_face.at[k], inv_sem.at[k])
            )
        for copy in copies:
            copy.start()

        places = []
        for k in range(levels):
            axis = "cut" if k < CUTLV else "sub"
            bits = lax.axis_size(axis).bit_length() - 1
            apart = bits - 1 - (k if k < CUTLV else k - CUTLV)
            me = lax.axis_index(axis)
            upper = lax.rem(lax.div(me, 1 << apart), 2)
            far = me + (1 - 2 * upper) * (1 << apart)
            places.append(({axis: far}, upper, 1 - upper))

        barrier = pltpu.get_barrier_semaphore()
        for target, _, _ in places:
            pl.semaphore_signal(barrier, inc=1, device_id=target, device_id_type=MESH)

        def down(row, first, height):
            shape = (height, row.shape[1])
            spots = (lax.broadcasted_iota(jnp.int32, shape, 0) + first).astype(INDEX)
            wanted = jnp.broadcast_to(row, shape).astype(INDEX)
            one, zero = jnp.bfloat16(1), jnp.bfloat16(0)
            return jnp.where(wanted == spots, one, zero)

        def build_slab(k):
            def step(i, carry):
                first = pl.multiple_of(i * CHUNK, CHUNK)
                p_t[k, pl.ds(first, CHUNK), :] = down(dofs[k], first, CHUNK)
                return carry

            lax.fori_loop(0, ndof // CHUNK, step, 0)

        def build_stars(target, row_of, count, height):
            def step(i, carry):
                first = pl.multiple_of(i * CHUNK, CHUNK)
                for j in range(count):
                    row = rows[row_of + j : row_of + j + 1, :]
                    target[pl.ds(first, CHUNK), j * pad : (j + 1) * pad] = down(row, first, CHUNK)
                return carry

            lax.fori_loop(0, height // CHUNK, step, 0)

        def build_face(k):
            build_stars(st_face.at[k], nint + k * slots, slots, joint)

        send, give = [], []
        for k, (target, own, far) in enumerate(places):
            send.append(
                pltpu.make_async_remote_copy(
                    src_ref=joined.at[k, own],
                    dst_ref=joined.at[k, own],
                    send_sem=send_sem.at[k],
                    recv_sem=recv_sem.at[k],
                    device_id=target,
                    device_id_type=MESH,
                )
            )
            give.append(
                pltpu.make_async_remote_copy(
                    src_ref=terms.at[k, far],
                    dst_ref=back.at[k],
                    send_sem=give_sem.at[k],
                    recv_sem=back_sem.at[k],
                    device_id=target,
                    device_id_type=MESH,
                )
            )

        res_t[...] = res[0, 0].T
        for k, (_, own, _) in enumerate(places):
            build_slab(k)
            if k == 1:
                pl.semaphore_wait(barrier, levels)
            if k >= 1:
                send[k - 1].start()
            mine = jnp.dot(res_t[...], p_t[k], preferred_element_type=jnp.float32)
            joined[k, own] = mine.astype(jnp.bfloat16)

        rows[...] = jnp.full(rows.shape, -1, jnp.int32)
        rows[0:nint, 0:star] = inner_idx[0, 0]
        for k in range(levels):
            for j in range(slots):
                at = nint + k * slots + j
                live = j < counts[0, 0, k]
                rows[at : at + 1, 0:star] = jnp.where(live, face_idx[k * slots + j], -1)
        pair[...] = jnp.zeros(pair.shape, jnp.bfloat16)
        send[levels - 1].start()

        def solve(picked, inverses, count):
            gathered[:, 0 : count * pad] = picked.astype(jnp.bfloat16)
            for j in range(count):
                solved = lax.dot_general(
                    inverses[j],
                    gathered[:, j * pad : j * pad + star],
                    (((1,), (1,)), ((), ())),
                    preferred_element_type=jnp.float32,
                )
                high, low = split_pair(solved)
                pair[j * pad : j * pad + star, 0:nrhs] = high
                pair[j * pad : j * pad + star, nrhs : 2 * nrhs] = low

        def face(k):
            _, own, far = places[k]
            send[k].wait_recv()
            copies[1 + k].wait()
            picked = jnp.dot(
                joined[k, 0], st_face[k, 0:slab, :], preferred_element_type=jnp.float32
            ) + jnp.dot(
                joined[k, 1], st_face[k, slab:joint, :], preferred_element_type=jnp.float32
            )
            solve(picked, inv_face.at[k], slots)
            for half in (far, own):
                at = pl.multiple_of(half * slab, slab)
                both = jnp.dot(
                    st_face[k, pl.ds(at, slab), :],
                    pair[0 : slots * pad],
                    preferred_element_type=jnp.float32,
                )
                terms[k, half] = both[:, :nrhs] + both[:, nrhs:]
            give[k].start()

        for k in early:
            build_face(k)
        build_stars(st_in, 0, nint, ndof)
        copies[0].wait()
        solve(
            jnp.dot(res_t[...], st_in[...], preferred_element_type=jnp.float32), inv_in, nint
        )
        acc[...] = jnp.dot(
            st_in[...], pair[0 : nint * pad], preferred_element_type=jnp.float32
        )
        for k in order:
            if k not in early:
                build_face(k)
            face(k)

        for k in finish:
            _, own, _ = places[k]
            give[k].wait_recv()
            high, low = split_pair(terms[k, own] + back[k])
            pair[0:slab, 0:nrhs] = high
            pair[0:slab, nrhs : 2 * nrhs] = low
            both = jnp.dot(p_t[k], pair[0:slab], preferred_element_type=jnp.float32)
            if k == finish[-1]:
                both = acc[...] + both
                out[0, 0] = both[:, :nrhs] + both[:, nrhs:]
            else:
                acc[...] += both
        for k in range(levels):
            send[k].wait_send()
            give[k].wait_send()

    return kernel


def on_device(
    residual, inner_inverse, inner_index, slab_dofs, face_inverse, face_index, face_count
):
    ndof, nrhs = residual.shape[2:]
    nint, star = inner_index.shape[2:]
    levels, slots = face_index.shape[2:4]
    slab = slab_dofs.shape[3]
    pad = round_up(star, LANES)
    joint = 2 * slab
    index_rows = round_up(nint + levels * slots, 8)
    early, order, finish = (0, 1, 2), (0, 1, 2, 3, 4), (2, 3, 4, 1, 0)
    kinds = jnp.bfloat16
    vmem = pl.BlockSpec(memory_space=pltpu.VMEM)
    anywhere = pl.BlockSpec(memory_space=pl.ANY)
    scalar = pl.BlockSpec(memory_space=pltpu.SMEM)
    most = max(nint, slots) * pad
    return pl.pallas_call(
        make_kernel(ndof, nrhs, nint, star, levels, slots, slab, early, order, finish),
        out_shape=jax.ShapeDtypeStruct(residual.shape, jnp.float32),
        in_specs=[vmem, anywhere, vmem, vmem, anywhere, vmem, scalar],
        out_specs=vmem,
        scratch_shapes=[
            pltpu.VMEM((nint, star, star), kinds),
            pltpu.VMEM((levels, slots, star, star), kinds),
            pltpu.VMEM((index_rows, pad), jnp.int32),
            pltpu.VMEM((nrhs, ndof), kinds),
            pltpu.VMEM((ndof, nint * pad), kinds),
            pltpu.VMEM((levels, joint, slots * pad), kinds),
            pltpu.VMEM((levels, ndof, slab), kinds),
            pltpu.VMEM((nrhs, most), kinds),
            pltpu.VMEM((max(most, slab), 2 * nrhs), kinds),
            pltpu.VMEM((levels, 2, nrhs, slab), kinds),
            pltpu.VMEM((levels, 2, slab, nrhs), jnp.float32),
            pltpu.VMEM((levels, slab, nrhs), jnp.float32),
            pltpu.VMEM((ndof, 2 * nrhs), jnp.float32),
            pltpu.SemaphoreType.DMA((levels + 1,)),
            pltpu.SemaphoreType.DMA((levels,)),
            pltpu.SemaphoreType.DMA((levels,)),
            pltpu.SemaphoreType.DMA((levels,)),
            pltpu.SemaphoreType.DMA((levels,)),
        ],
        compiler_params=pltpu.CompilerParams(
            collective_id=0, has_side_effects=True, vmem_limit_bytes=64000000
        ),
    )(
        residual,
        inner_inverse,
        inner_index,
        slab_dofs.reshape(levels, 1, slab),
        face_inverse,
        face_index.reshape(levels * slots, 1, star),
        face_count,
    )


def solution(mesh):
    return jax.shard_map(
        on_device,
        mesh=mesh,
        in_specs=(
            P("cut", "sub", None, None),
            P("cut", "sub", None, None, None),
            P("cut", "sub", None, None),
            P("cut", "sub", None, None),
            P("cut", "sub", None, None, None, None),
            P("cut", "sub", None, None, None),
            P("cut", "sub", None),
        ),
        out_specs=P("cut", "sub", None, None),
        check_vma=False,
    )
```

```python
import jax
import jax.numpy as jnp
from jax import lax
from jax.experimental import pallas as pl
from jax.experimental.pallas import tpu as pltpu
from jax.sharding import PartitionSpec as P

CUTLV = 3
LANES = 128
CHUNK = 128
INDEX = jnp.int16
STEPS = 32766.0
FLOOR = 1e-30
MESH = pl.DeviceIdType.MESH


def round_up(value, step):
    return (value + step - 1) // step * step


def split_pair(values):
    high = values.astype(jnp.bfloat16)
    low = (values - high.astype(jnp.float32)).astype(jnp.bfloat16)
    return high, low


def make_kernel(ndof, nrhs, nint, star, levels, slots, slab, early, order, finish):
    pad = round_up(star, LANES)
    joint = 2 * slab

    def kernel(
        res, inner_inv, inner_idx, dofs, face_inv, face_idx, counts, out,
        inv_in, inv_face, rows, res_t, st_in, st_face, p_t,
        gathered, pair, joined, kept, terms, peaks, back, back_peaks, acc,
        inv_sem, send_sem, recv_sem, give_sem, back_sem, peak_sem, back_peak_sem,
    ):
        copies = [pltpu.make_async_copy(inner_inv.at[0, 0], inv_in, inv_sem.at[levels])]
        for k in range(levels):
            copies.append(
                pltpu.make_async_copy(face_inv.at[0, 0, k], inv_face.at[k], inv_sem.at[k])
            )
        for copy in copies:
            copy.start()

        places = []
        for k in range(levels):
            axis = "cut" if k < CUTLV else "sub"
            bits = lax.axis_size(axis).bit_length() - 1
            apart = bits - 1 - (k if k < CUTLV else k - CUTLV)
            me = lax.axis_index(axis)
            upper = lax.rem(lax.div(me, 1 << apart), 2)
            far = me + (1 - 2 * upper) * (1 << apart)
            places.append(({axis: far}, upper, 1 - upper))

        barrier = pltpu.get_barrier_semaphore()
        for target, _, _ in places:
            pl.semaphore_signal(barrier, inc=1, device_id=target, device_id_type=MESH)

        def down(row, first, height):
            shape = (height, row.shape[1])
            spots = (lax.broadcasted_iota(jnp.int32, shape, 0) + first).astype(INDEX)
            wanted = jnp.broadcast_to(row, shape).astype(INDEX)
            one, zero = jnp.bfloat16(1), jnp.bfloat16(0)
            return jnp.where(wanted == spots, one, zero)

        def build_slab(k):
            def step(i, carry):
                first = pl.multiple_of(i * CHUNK, CHUNK)
                p_t[k, pl.ds(first, CHUNK), :] = down(dofs[k], first, CHUNK)
                return carry

            lax.fori_loop(0, ndof // CHUNK, step, 0)

        def build_stars(target, row_of, count, height):
            def step(i, carry):
                first = pl.multiple_of(i * CHUNK, CHUNK)
                for j in range(count):
                    row = rows[row_of + j : row_of + j + 1, :]
                    target[pl.ds(first, CHUNK), j * pad : (j + 1) * pad] = down(row, first, CHUNK)
                return carry

            lax.fori_loop(0, height // CHUNK, step, 0)

        def build_face(k):
            build_stars(st_face.at[k], nint + k * slots, slots, joint)

        send, give, give_peak = [], [], []
        for k, (target, own, far) in enumerate(places):
            send.append(
                pltpu.make_async_remote_copy(
                    src_ref=joined.at[k, own],
                    dst_ref=joined.at[k, own],
                    send_sem=send_sem.at[k],
                    recv_sem=recv_sem.at[k],
                    device_id=target,
                    device_id_type=MESH,
                )
            )
            give.append(
                pltpu.make_async_remote_copy(
                    src_ref=terms.at[k],
                    dst_ref=back.at[k],
                    send_sem=give_sem.at[k],
                    recv_sem=back_sem.at[k],
                    device_id=target,
                    device_id_type=MESH,
                )
            )

            give_peak.append(
                pltpu.make_async_remote_copy(
                    src_ref=peaks.at[k],
                    dst_ref=back_peaks.at[k],
                    send_sem=peak_sem.at[k],
                    recv_sem=back_peak_sem.at[k],
                    device_id=target,
                    device_id_type=MESH,
                )
            )

        res_t[...] = res[0, 0].T
        for k, (_, own, _) in enumerate(places):
            build_slab(k)
            if k == 1:
                pl.semaphore_wait(barrier, levels)
            if k >= 1:
                send[k - 1].start()
            mine = jnp.dot(res_t[...], p_t[k], preferred_element_type=jnp.float32)
            joined[k, own] = mine.astype(jnp.bfloat16)

        rows[...] = jnp.full(rows.shape, -1, jnp.int32)
        rows[0:nint, 0:star] = inner_idx[0, 0]
        for k in range(levels):
            for j in range(slots):
                at = nint + k * slots + j
                live = j < counts[0, 0, k]
                rows[at : at + 1, 0:star] = jnp.where(live, face_idx[k * slots + j], -1)
        pair[...] = jnp.zeros(pair.shape, jnp.bfloat16)
        send[levels - 1].start()

        def solve(picked, inverses, count):
            gathered[:, 0 : count * pad] = picked.astype(jnp.bfloat16)
            for j in range(count):
                solved = lax.dot_general(
                    inverses[j],
                    gathered[:, j * pad : j * pad + star],
                    (((1,), (1,)), ((), ())),
                    preferred_element_type=jnp.float32,
                )
                high, low = split_pair(solved)
                pair[j * pad : j * pad + star, 0:nrhs] = high
                pair[j * pad : j * pad + star, nrhs : 2 * nrhs] = low

        def face(k):
            _, own, far = places[k]
            send[k].wait_recv()
            copies[1 + k].wait()
            picked = jnp.dot(
                joined[k, 0], st_face[k, 0:slab, :], preferred_element_type=jnp.float32
            ) + jnp.dot(
                joined[k, 1], st_face[k, slab:joint, :], preferred_element_type=jnp.float32
            )
            solve(picked, inv_face.at[k], slots)
            def half_terms(half):
                at = pl.multiple_of(half * slab, slab)
                both = jnp.dot(
                    st_face[k, pl.ds(at, slab), :],
                    pair[0 : slots * pad],
                    preferred_element_type=jnp.float32,
                )
                return both[:, :nrhs] + both[:, nrhs:]

            given = half_terms(far)
            peak = jnp.maximum(jnp.max(jnp.abs(given), axis=0, keepdims=True), FLOOR)
            peaks[k] = jnp.broadcast_to(peak, peaks.shape[1:])
            terms[k] = jnp.round(given * (STEPS / peak)).astype(jnp.int32).astype(jnp.int16)
            kept[k] = half_terms(own)
            give_peak[k].start()
            give[k].start()

        for k in early:
            build_face(k)
        build_stars(st_in, 0, nint, ndof)
        copies[0].wait()
        solve(
            jnp.dot(res_t[...], st_in[...], preferred_element_type=jnp.float32), inv_in, nint
        )
        acc[...] = jnp.dot(
            st_in[...], pair[0 : nint * pad], preferred_element_type=jnp.float32
        )
        for k in order:
            if k not in early:
                build_face(k)
            face(k)

        for k in finish:
            give_peak[k].wait_recv()
            give[k].wait_recv()
            unit = back_peaks[k, 0:1, :] * (1.0 / STEPS)
            returned = back[k].astype(jnp.int32).astype(jnp.float32) * unit
            high, low = split_pair(kept[k] + returned)
            pair[0:slab, 0:nrhs] = high
            pair[0:slab, nrhs : 2 * nrhs] = low
            both = jnp.dot(p_t[k], pair[0:slab], preferred_element_type=jnp.float32)
            if k == finish[-1]:
                both = acc[...] + both
                out[0, 0] = both[:, :nrhs] + both[:, nrhs:]
            else:
                acc[...] += both
        for k in range(levels):
            send[k].wait_send()
            give[k].wait_send()
            give_peak[k].wait_send()

    return kernel


def on_device(
    residual, inner_inverse, inner_index, slab_dofs, face_inverse, face_index, face_count
):
    ndof, nrhs = residual.shape[2:]
    nint, star = inner_index.shape[2:]
    levels, slots = face_index.shape[2:4]
    slab = slab_dofs.shape[3]
    pad = round_up(star, LANES)
    joint = 2 * slab
    index_rows = round_up(nint + levels * slots, 8)
    early, order, finish = (0, 1, 2), (0, 1, 2, 3, 4), (2, 3, 4, 1, 0)
    kinds = jnp.bfloat16
    vmem = pl.BlockSpec(memory_space=pltpu.VMEM)
    anywhere = pl.BlockSpec(memory_space=pl.ANY)
    scalar = pl.BlockSpec(memory_space=pltpu.SMEM)
    most = max(nint, slots) * pad
    return pl.pallas_call(
        make_kernel(ndof, nrhs, nint, star, levels, slots, slab, early, order, finish),
        out_shape=jax.ShapeDtypeStruct(residual.shape, jnp.float32),
        in_specs=[vmem, anywhere, vmem, vmem, anywhere, vmem, scalar],
        out_specs=vmem,
        scratch_shapes=[
            pltpu.VMEM((nint, star, star), kinds),
            pltpu.VMEM((levels, slots, star, star), kinds),
            pltpu.VMEM((index_rows, pad), jnp.int32),
            pltpu.VMEM((nrhs, ndof), kinds),
            pltpu.VMEM((ndof, nint * pad), kinds),
            pltpu.VMEM((levels, joint, slots * pad), kinds),
            pltpu.VMEM((levels, ndof, slab), kinds),
            pltpu.VMEM((nrhs, most), kinds),
            pltpu.VMEM((max(most, slab), 2 * nrhs), kinds),
            pltpu.VMEM((levels, 2, nrhs, slab), kinds),
            pltpu.VMEM((levels, slab, nrhs), jnp.float32),
            pltpu.VMEM((levels, slab, nrhs), jnp.int16),
            pltpu.VMEM((levels, 8, nrhs), jnp.float32),
            pltpu.VMEM((levels, slab, nrhs), jnp.int16),
            pltpu.VMEM((levels, 8, nrhs), jnp.float32),
            pltpu.VMEM((ndof, 2 * nrhs), jnp.float32),
            pltpu.SemaphoreType.DMA((levels + 1,)),
            pltpu.SemaphoreType.DMA((levels,)),
            pltpu.SemaphoreType.DMA((levels,)),
            pltpu.SemaphoreType.DMA((levels,)),
            pltpu.SemaphoreType.DMA((levels,)),
            pltpu.SemaphoreType.DMA((levels,)),
            pltpu.SemaphoreType.DMA((levels,)),
        ],
        compiler_params=pltpu.CompilerParams(
            collective_id=0, has_side_effects=True, vmem_limit_bytes=64000000
        ),
    )(
        residual,
        inner_inverse,
        inner_index,
        slab_dofs.reshape(levels, 1, slab),
        face_inverse,
        face_index.reshape(levels * slots, 1, star),
        face_count,
    )


def solution(mesh):
    return jax.shard_map(
        on_device,
        mesh=mesh,
        in_specs=(
            P("cut", "sub", None, None),
            P("cut", "sub", None, None, None),
            P("cut", "sub", None, None),
            P("cut", "sub", None, None),
            P("cut", "sub", None, None, None, None),
            P("cut", "sub", None, None, None),
            P("cut", "sub", None),
        ),
        out_specs=P("cut", "sub", None, None),
        check_vma=False,
    )
```

```python
import jax
import jax.numpy as jnp
from jax import lax
from jax.experimental import pallas as pl
from jax.experimental.pallas import tpu as pltpu
from jax.sharding import PartitionSpec as P

CUTLV = 3
LANES = 128
CHUNK = 128
INDEX = jnp.int16
STEPS = 32766.0
FLOOR = 1e-30
MESH = pl.DeviceIdType.MESH


def round_up(value, step):
    return (value + step - 1) // step * step


def split_pair(values):
    high = values.astype(jnp.bfloat16)
    low = (values - high.astype(jnp.float32)).astype(jnp.bfloat16)
    return high, low


def make_kernel(ndof, nrhs, nint, star, levels, slots, slab, early, order, finish):
    pad = round_up(star, LANES)
    joint = 2 * slab

    def kernel(
        res, inner_inv, inner_idx, dofs, face_inv, face_idx, counts, out,
        inv_in, inv_face, rows, res_t, st_in, st_face, p_t,
        gathered, pair, joined, kept, terms, peaks, back, back_peaks, acc,
        inv_sem, send_sem, recv_sem, give_sem, back_sem, peak_sem, back_peak_sem,
    ):
        copies = [pltpu.make_async_copy(inner_inv.at[0, 0], inv_in, inv_sem.at[levels])]
        for k in range(levels):
            copies.append(
                pltpu.make_async_copy(face_inv.at[0, 0, k], inv_face.at[k], inv_sem.at[k])
            )
        for copy in copies:
            copy.start()

        places = []
        for k in range(levels):
            axis = "cut" if k < CUTLV else "sub"
            bits = lax.axis_size(axis).bit_length() - 1
            apart = bits - 1 - (k if k < CUTLV else k - CUTLV)
            me = lax.axis_index(axis)
            upper = lax.rem(lax.div(me, 1 << apart), 2)
            far = me + (1 - 2 * upper) * (1 << apart)
            places.append(({axis: far}, upper, 1 - upper))

        barrier = pltpu.get_barrier_semaphore()
        for target, _, _ in places:
            pl.semaphore_signal(barrier, inc=1, device_id=target, device_id_type=MESH)

        def down(row, first, height):
            shape = (height, row.shape[1])
            spots = (lax.broadcasted_iota(jnp.int32, shape, 0) + first).astype(INDEX)
            wanted = jnp.broadcast_to(row, shape).astype(INDEX)
            one, zero = jnp.bfloat16(1), jnp.bfloat16(0)
            return jnp.where(wanted == spots, one, zero)

        def build_slab(k):
            def step(i, carry):
                first = pl.multiple_of(i * CHUNK, CHUNK)
                p_t[k, pl.ds(first, CHUNK), :] = down(dofs[k], first, CHUNK)
                return carry

            lax.fori_loop(0, ndof // CHUNK, step, 0)

        def build_stars(target, row_of, count, height):
            def step(i, carry):
                first = pl.multiple_of(i * CHUNK, CHUNK)
                for j in range(count):
                    row = rows[row_of + j : row_of + j + 1, :]
                    target[pl.ds(first, CHUNK), j * pad : (j + 1) * pad] = down(row, first, CHUNK)
                return carry

            lax.fori_loop(0, height // CHUNK, step, 0)

        def build_face(k):
            build_stars(st_face.at[k], nint + k * slots, slots, joint)

        send, give, give_peak = [], [], []
        for k, (target, own, far) in enumerate(places):
            send.append(
                pltpu.make_async_remote_copy(
                    src_ref=joined.at[k, own],
                    dst_ref=joined.at[k, own],
                    send_sem=send_sem.at[k],
                    recv_sem=recv_sem.at[k],
                    device_id=target,
                    device_id_type=MESH,
                )
            )
            give.append(
                pltpu.make_async_remote_copy(
                    src_ref=terms.at[k],
                    dst_ref=back.at[k],
                    send_sem=give_sem.at[k],
                    recv_sem=back_sem.at[k],
                    device_id=target,
                    device_id_type=MESH,
                )
            )

            give_peak.append(
                pltpu.make_async_remote_copy(
                    src_ref=peaks.at[k],
                    dst_ref=back_peaks.at[k],
                    send_sem=peak_sem.at[k],
                    recv_sem=back_peak_sem.at[k],
                    device_id=target,
                    device_id_type=MESH,
                )
            )

        res_t[...] = res[0, 0].T
        for k, (_, own, _) in enumerate(places):
            build_slab(k)
            if k == 1:
                pl.semaphore_wait(barrier, levels)
            if k >= 1:
                send[k - 1].start()
            mine = jnp.dot(res_t[...], p_t[k], preferred_element_type=jnp.float32)
            joined[k, own] = mine.astype(jnp.bfloat16)

        rows[...] = jnp.full(rows.shape, -1, jnp.int32)
        rows[0:nint, 0:star] = inner_idx[0, 0]
        for k in range(levels):
            for j in range(slots):
                at = nint + k * slots + j
                live = j < counts[0, 0, k]
                rows[at : at + 1, 0:star] = jnp.where(live, face_idx[k * slots + j], -1)
        pair[...] = jnp.zeros(pair.shape, jnp.bfloat16)
        send[levels - 1].start()

        def solve(picked, inverses, count):
            gathered[:, 0 : count * pad] = picked.astype(jnp.bfloat16)
            for j in range(count):
                solved = lax.dot_general(
                    inverses[j],
                    gathered[:, j * pad : j * pad + star],
                    (((1,), (1,)), ((), ())),
                    preferred_element_type=jnp.float32,
                )
                high, low = split_pair(solved)
                pair[j * pad : j * pad + star, 0:nrhs] = high
                pair[j * pad : j * pad + star, nrhs : 2 * nrhs] = low

        def face(k):
            _, own, far = places[k]
            send[k].wait_recv()
            copies[1 + k].wait()
            picked = jnp.dot(
                joined[k, 0], st_face[k, 0:slab, :], preferred_element_type=jnp.float32
            ) + jnp.dot(
                joined[k, 1], st_face[k, slab:joint, :], preferred_element_type=jnp.float32
            )
            solve(picked, inv_face.at[k], slots)
            def half_terms(half):
                at = pl.multiple_of(half * slab, slab)
                both = jnp.dot(
                    st_face[k, pl.ds(at, slab), :],
                    pair[0 : slots * pad],
                    preferred_element_type=jnp.float32,
                )
                return both[:, :nrhs] + both[:, nrhs:]

            given = half_terms(far)
            peak = jnp.maximum(jnp.max(jnp.abs(given), axis=0, keepdims=True), FLOOR)
            peaks[k] = jnp.broadcast_to(peak, peaks.shape[1:])
            terms[k] = jnp.round(given * (STEPS / peak)).astype(jnp.int32).astype(jnp.int16)
            kept[k] = half_terms(own)
            give_peak[k].start()
            give[k].start()

        for k in early:
            build_face(k)
        build_stars(st_in, 0, nint, ndof)
        copies[0].wait()
        solve(
            jnp.dot(res_t[...], st_in[...], preferred_element_type=jnp.float32), inv_in, nint
        )
        acc[...] = jnp.dot(
            st_in[...], pair[0 : nint * pad], preferred_element_type=jnp.float32
        )
        for k in order:
            if k not in early:
                build_face(k)
            face(k)

        for k in finish:
            give_peak[k].wait_recv()
            give[k].wait_recv()
            unit = back_peaks[k, 0:1, :] * (1.0 / STEPS)
            returned = back[k].astype(jnp.int32).astype(jnp.float32) * unit
            high, low = split_pair(kept[k] + returned)
            pair[0:slab, 0:nrhs] = high
            pair[0:slab, nrhs : 2 * nrhs] = low
            both = jnp.dot(p_t[k], pair[0:slab], preferred_element_type=jnp.float32)
            if k == finish[-1]:
                both = acc[...] + both
                out[0, 0] = both[:, :nrhs] + both[:, nrhs:]
            else:
                acc[...] += both
        for k in range(levels):
            send[k].wait_send()
            give[k].wait_send()
            give_peak[k].wait_send()

    return kernel


def on_device(
    residual, inner_inverse, inner_index, slab_dofs, face_inverse, face_index, face_count
):
    ndof, nrhs = residual.shape[2:]
    nint, star = inner_index.shape[2:]
    levels, slots = face_index.shape[2:4]
    slab = slab_dofs.shape[3]
    pad = round_up(star, LANES)
    joint = 2 * slab
    index_rows = round_up(nint + levels * slots, 8)
    early, order, finish = (0, 1), (4, 3, 0, 1, 2), (4, 3, 0, 1, 2)
    kinds = jnp.bfloat16
    vmem = pl.BlockSpec(memory_space=pltpu.VMEM)
    anywhere = pl.BlockSpec(memory_space=pl.ANY)
    scalar = pl.BlockSpec(memory_space=pltpu.SMEM)
    most = max(nint, slots) * pad
    return pl.pallas_call(
        make_kernel(ndof, nrhs, nint, star, levels, slots, slab, early, order, finish),
        out_shape=jax.ShapeDtypeStruct(residual.shape, jnp.float32),
        in_specs=[vmem, anywhere, vmem, vmem, anywhere, vmem, scalar],
        out_specs=vmem,
        scratch_shapes=[
            pltpu.VMEM((nint, star, star), kinds),
            pltpu.VMEM((levels, slots, star, star), kinds),
            pltpu.VMEM((index_rows, pad), jnp.int32),
            pltpu.VMEM((nrhs, ndof), kinds),
            pltpu.VMEM((ndof, nint * pad), kinds),
            pltpu.VMEM((levels, joint, slots * pad), kinds),
            pltpu.VMEM((levels, ndof, slab), kinds),
            pltpu.VMEM((nrhs, most), kinds),
            pltpu.VMEM((max(most, slab), 2 * nrhs), kinds),
            pltpu.VMEM((levels, 2, nrhs, slab), kinds),
            pltpu.VMEM((levels, slab, nrhs), jnp.float32),
            pltpu.VMEM((levels, slab, nrhs), jnp.int16),
            pltpu.VMEM((levels, 8, nrhs), jnp.float32),
            pltpu.VMEM((levels, slab, nrhs), jnp.int16),
            pltpu.VMEM((levels, 8, nrhs), jnp.float32),
            pltpu.VMEM((ndof, 2 * nrhs), jnp.float32),
            pltpu.SemaphoreType.DMA((levels + 1,)),
            pltpu.SemaphoreType.DMA((levels,)),
            pltpu.SemaphoreType.DMA((levels,)),
            pltpu.SemaphoreType.DMA((levels,)),
            pltpu.SemaphoreType.DMA((levels,)),
            pltpu.SemaphoreType.DMA((levels,)),
            pltpu.SemaphoreType.DMA((levels,)),
        ],
        compiler_params=pltpu.CompilerParams(
            collective_id=0, has_side_effects=True, vmem_limit_bytes=64000000
        ),
    )(
        residual,
        inner_inverse,
        inner_index,
        slab_dofs.reshape(levels, 1, slab),
        face_inverse,
        face_index.reshape(levels * slots, 1, star),
        face_count,
    )


def solution(mesh):
    return jax.shard_map(
        on_device,
        mesh=mesh,
        in_specs=(
            P("cut", "sub", None, None),
            P("cut", "sub", None, None, None),
            P("cut", "sub", None, None),
            P("cut", "sub", None, None),
            P("cut", "sub", None, None, None, None),
            P("cut", "sub", None, None, None),
            P("cut", "sub", None),
        ),
        out_specs=P("cut", "sub", None, None),
        check_vma=False,
    )
```
